32 devices in a mesh: ep: 4 (over x, core), tp: 8 (over z, y).
Axes of the slice: x: 2, y: 2, z: 4, core: 2. Of those that a mesh axis runs over, the one named last changes fastest.
Arguments:
- layer_input: bfloat16 [1024, 4096], P('ep', 'tp'), may hold values from -6 to 6
- out_grad: bfloat16 [1024, 4096], P('ep', 'tp'), may hold values from -6 to 6
- route: int32 [1024, 2], P('ep'), may hold values from 0 to 3, all different within a row; in each aligned block of 256 rows (0 to 255, 256 to 511, ...) at most 192 rows name the same one
- gate_share: float32 [1024, 2], P('ep'), may hold values from 0.2 to 1
- gate_weight: bfloat16 [4, 4096, 14336], P('ep', None, 'tp'), may hold values from -0.125 to 0.125
- up_weight: bfloat16 [4, 4096, 14336], P('ep', None, 'tp'), may hold values from -0.125 to 0.125
- down_weight: bfloat16 [4, 14336, 4096], P('ep', 'tp'), may hold values from -0.046875 to 0.046875
Outputs:
- input_grad: bfloat16 [1024, 4096], P('ep', 'tp')
The draws below stay inside these ranges and needn't reach their ends.
Inputs may be any that keep to these rules, and one draw needn't show every extreme that they name: `route`: each row names 2 different experts. In each aligned block of 256 rows (the rows of one index of ep) no expert is named by more than 192 rows, a bound that some block reaches.
All inputs are finite; a program needn't handle non-finite values.
Results may differ from the reference program's by a relative error of at most 0.0057.
Values may be sent and summed in bfloat16 or wider, within the bound.
A program may use at most 320 MiB of HBM per device.

```python
import math
import jax
import jax.numpy as jnp
import numpy as np
from jax import lax

D = 4096
FF = 14336
TOP = 2
TOK_EP = 256
EXPERTS = 4
CAP = 192
TOKENS = 1024
N_EP = 4


def with_spikes(result, rng, source, target, blocks, factor):
    def block_of(dim):
        return (jnp.arange(result.shape[dim]) // (result.shape[dim] // blocks)).reshape((-1,) + (1,) * (result.ndim - 1 - dim))

    first = jax.random.permutation(rng, blocks)[block_of(target)]
    second = (block_of(target) + blocks // 2) % blocks
    return jnp.where((block_of(source) == first) | (block_of(source) == second), factor * result, result)


def shard_levels(key, extent, shards, low, high):
    loudness = 1.0
    for dim, blocks in shards:
        heights = jax.random.uniform(jax.random.fold_in(jax.random.fold_in(key, 6), dim), (blocks,), jnp.float32, low / len(shards), high / len(shards))
        loudness = loudness * jnp.repeat(jnp.exp(heights), extent[dim] // blocks).reshape((-1,) + (1,) * (len(extent) - 1 - dim))
    return loudness


def deal_out(rng, own, number, rows, count, top, most, lean):
    sequence = jax.random.permutation(rng, count)
    heavy_load, common = portions_of(count, rows * top, most, lean, True), portions_of(count, rows * top, most, lean, False)
    places = jnp.arange(count)

    def named(tallies, turn):
        used = int((tallies > 0).sum())
        fixed = max(1, used // 4)
        shifted = fixed + (places - fixed + turn * (used - fixed)) % max(1, count - fixed)
        return jnp.zeros((count,), jnp.int32).at[sequence[jnp.where(places < fixed, places, shifted)]].set(jnp.asarray(tallies, jnp.int32))

    tallies = jnp.where(number % 4 == 0, named(heavy_load, number // 4), named(common, number - number // 4 - 1))
    mixed = jax.random.permutation(jax.random.fold_in(own, 3), count)
    donor, receiver = mixed[0:count // 2 * 2:2], mixed[1:count // 2 * 2:2]
    margin = jnp.minimum(tallies[donor] - 1, most - tallies[receiver]) // 2
    margin = jnp.where((donor == sequence[0]) | (receiver == sequence[0]) | (tallies[receiver] == 0), 0, jnp.maximum(margin, 0))
    shifted = jax.random.randint(jax.random.fold_in(own, 4), (count // 2,), 0, 1 << 20) % (margin + 1)
    tallies = tallies.at[donor].add(-shifted).at[receiver].add(shifted)
    items = jnp.searchsorted(jnp.cumsum(tallies), jnp.arange(rows * top), side="right").astype(jnp.int32)
    grid = items.reshape(top, rows).T
    grid = grid[jax.random.permutation(jax.random.fold_in(own, 1), rows)]
    turn = jax.random.randint(jax.random.fold_in(own, 2), (rows, 1), 0, top)
    return jnp.take_along_axis(grid, (jnp.arange(top)[None, :] + turn) % top, axis=1)


def portions_of(count, total, most, lean, full):
    loads = [(1 << 20) // math.isqrt(standing ** lean) + 1 for standing in range(1, count + 1)]
    largest = most if full else min(most, max(-(-total // count), total * loads[0] // sum(loads)))
    least = 1 if total - largest >= count - 1 else 0
    holding, spare = [largest] + [least] * (count - 1), total - largest - least * (count - 1)
    while spare > 0:
        free = [i for i in range(1, count) if holding[i] < largest] or [i for i in range(1, count) if holding[i] < most]
        whole, budget = sum([loads[i] for i in free]), spare
        for i in free:
            addition = min(most - holding[i], max(1, budget * loads[i] // whole), spare)
            holding[i] = holding[i] + addition
            spare = spare - addition
    return np.array(holding)


def centred(stream_key, shape, width, limit, split=(), held_as=jnp.bfloat16):
    values = width * jax.random.normal(stream_key, shape, jnp.float32)
    if split:
        values = values * shard_levels(stream_key, shape, split, -0.22, 0.18)
    return jnp.clip(values, -limit, limit).astype(held_as)


def gaussian_with(stream_key, shape, deviation, limit, pieces, heavy, kind=jnp.bfloat16):
    values = deviation * jax.random.normal(stream_key, shape, jnp.float32)
    if pieces:
        values = values * shard_levels(stream_key, shape, pieces, -0.22, 0.18)
    return jnp.clip(with_spikes(values, jax.random.fold_in(stream_key, 3), *heavy), -limit, limit).astype(kind)


def setup_inputs(seed: int = 0) -> dict:
    seeds = jax.random.split(jax.random.key(seed), 8)
    layer_input = centred(seeds[0], (TOKENS, D), 1.0, 6.0, ((0, 4), (1, 8)))
    out_grad = centred(seeds[1], (TOKENS, D), 1.0, 6.0, ((0, 4), (1, 8)))
    route_keys = jax.random.split(jax.random.fold_in(seeds[2], 1), TOKENS // TOK_EP)
    route_turns = jax.random.permutation(jax.random.fold_in(seeds[2], 3), TOKENS // TOK_EP)
    route = jax.vmap(lambda own, number: deal_out(jax.random.fold_in(seeds[2], 2), own, number, TOK_EP, EXPERTS, TOP, CAP, 2))(route_keys, route_turns).reshape((TOKENS, TOP))
    gate_share = jnp.clip(0.2 + 0.8 * jax.random.uniform(seeds[3], (TOKENS, TOP), jnp.float32) ** shard_levels(seeds[3], (TOKENS, TOP), ((0, 4),), -0.2, 0.2), 0.2, 1.0)
    gate_weight = gaussian_with(seeds[4], (EXPERTS, D, FF), D ** -0.5, 0.125, ((0, 4), (2, 8)), (2, 1, 8, 2.0))
    up_weight = gaussian_with(seeds[5], (EXPERTS, D, FF), D ** -0.5, 0.125, ((0, 4), (2, 8)), (2, 1, 8, 2.0))
    down_weight = centred(seeds[6], (EXPERTS, FF, D), FF ** -0.5, 0.046875, ((0, 4), (1, 8)))
    return {"layer_input": layer_input, "out_grad": out_grad, "route": route, "gate_share": gate_share, "gate_weight": gate_weight, "up_weight": up_weight, "down_weight": down_weight}


def slot_positions(blocks):
    onehot = (blocks[..., None] == jnp.arange(EXPERTS, dtype=jnp.int32)).astype(jnp.int32).sum(axis=2)
    before = jnp.cumsum(onehot, axis=1) - onehot
    return jnp.take_along_axis(before, blocks, axis=2).astype(jnp.int32)


def expert_rows(gate_matrix, up_matrix, down_matrix, inputs, grads):
    gate_act = jnp.dot(inputs, gate_matrix, preferred_element_type=jnp.float32)
    up_act = jnp.dot(inputs, up_matrix, preferred_element_type=jnp.float32)
    hidden_grad = lax.dot_general(grads, down_matrix, (((1,), (1,)), ((), ())), preferred_element_type=jnp.float32)
    sigma = jax.nn.sigmoid(gate_act)
    slope = sigma * (1.0 + gate_act * (1.0 - sigma))
    gate_grad = (hidden_grad * up_act * slope).astype(jnp.bfloat16)
    up_grad = (hidden_grad * gate_act * sigma).astype(jnp.bfloat16)
    total = lax.dot_general(gate_grad, gate_matrix, (((1,), (1,)), ((), ())), preferred_element_type=jnp.float32)
    total = total + lax.dot_general(up_grad, up_matrix, (((1,), (1,)), ((), ())), preferred_element_type=jnp.float32)
    return total.astype(jnp.bfloat16)


def reference(layer_input, out_grad, route, gate_share, gate_weight, up_weight, down_weight):
    blocks = route.reshape(N_EP, TOK_EP, TOP)
    position = slot_positions(blocks)
    flat = blocks * CAP + position
    owner = jnp.broadcast_to(jnp.arange(TOK_EP, dtype=jnp.int32)[None, :, None], flat.shape)
    block_index = jnp.broadcast_to(jnp.arange(N_EP, dtype=jnp.int32)[:, None, None], flat.shape)
    inverse = jnp.full((N_EP, EXPERTS * CAP), TOK_EP, jnp.int32)
    inverse = inverse.at[block_index.reshape(-1), flat.reshape(-1)].set(owner.reshape(-1))
    inverse = inverse.reshape(N_EP, EXPERTS, CAP)

    def one_expert(expert):
        local = lax.dynamic_index_in_dim(inverse, expert, 1, keepdims=False)
        valid = (local < TOK_EP).reshape(-1)[:, None]
        rows = (jnp.arange(N_EP, dtype=jnp.int32)[:, None] * TOK_EP + jnp.minimum(local, TOK_EP - 1)).reshape(-1)
        zero_value = jnp.zeros((), layer_input.dtype)
        inputs = jnp.where(valid, jnp.take(layer_input, rows, axis=0), zero_value)
        grads = jnp.where(valid, jnp.take(out_grad, rows, axis=0), zero_value)
        gate_matrix = lax.dynamic_index_in_dim(gate_weight, expert, 0, keepdims=False)
        up_matrix = lax.dynamic_index_in_dim(up_weight, expert, 0, keepdims=False)
        down_matrix = lax.dynamic_index_in_dim(down_weight, expert, 0, keepdims=False)
        return expert_rows(gate_matrix, up_matrix, down_matrix, inputs, grads)

    returned = lax.map(one_expert, jnp.arange(EXPERTS, dtype=jnp.int32))
    returned = returned.reshape(EXPERTS, N_EP, CAP, D)
    picked = returned[blocks, block_index, position]
    shares = gate_share.reshape(N_EP, TOK_EP, TOP)[..., None]
    combined = jnp.sum(picked.astype(jnp.float32) * shares, axis=2)
    return combined.reshape(TOKENS, D).astype(jnp.bfloat16)
```

```python
import functools

import jax
import jax.numpy as jnp
from jax import lax
from jax.experimental import pallas as pl
from jax.experimental.pallas import tpu as pltpu
from jax.sharding import PartitionSpec as P

CORES = 2
TILE = 256
VMEM_BYTES = 67_043_328
NT = (((1,), (1,)), ((), ()))
MESH = pl.DeviceIdType.MESH
UP, DOWN, ACROSS_X, ACROSS_Y, SIBLING, ACROSS_BOTH = range(6)


def pick(table, index):
    value = jnp.int32(table[-1])
    for i in range(len(table) - 1):
        value = jnp.where(index == i, jnp.int32(table[i]), value)
    return value


class Place:
    def __init__(self, deep):
        ep, tp = lax.axis_index("ep"), lax.axis_index("tp")
        self.deep = deep
        self.x, self.core = ep // CORES, ep % CORES
        self.z, self.y = tp // 2, tp % 2
        self.ep, self.tp = ep, tp

    def device(self, way):
        ep, tp = self.ep, self.tp
        if way == SIBLING:
            return (self.x * CORES + 1 - self.core, tp)
        if way == ACROSS_X:
            return ((1 - self.x) * CORES + self.core, tp)
        if way == ACROSS_BOTH:
            return ((1 - self.x) * CORES + 1 - self.core, tp)
        if way == ACROSS_Y:
            return (ep, self.z * 2 + 1 - self.y)
        return (ep, tp + 2 if way == UP else tp - 2)

    def greet(self):
        barrier = pltpu.get_barrier_semaphore()

        def signal(way):
            pl.semaphore_signal(barrier, inc=1, device_id=self.device(way), device_id_type=MESH)

        ways = (SIBLING, ACROSS_X, ACROSS_Y, ACROSS_BOTH)
        for way in ways:
            signal(way)
        pl.when(self.z < self.deep - 1)(lambda: signal(UP))
        pl.when(self.z > 0)(lambda: signal(DOWN))
        lines = (self.z > 0).astype(jnp.int32) + (self.z < self.deep - 1).astype(jnp.int32)
        pl.semaphore_wait(barrier, len(ways) + lines)


def near_first(deep):
    return [sorted(range(deep), key=lambda other: (abs(other - z), other)) for z in range(deep)]


def gather_kernel(deep, x_ref, g_ref, s_ref, wg_ref, wu_ref, wd_ref, act_ref, share_ref,
                  land, share_land, acc, weights_a, weights_d, stage,
                  send, recv, half, share_sems, own_sems, weight_sems, out_sems):
    here = Place(deep)
    x, y, z, core = here.x, here.y, here.z, here.core
    rows, width = x_ref.shape
    hidden = wg_ref.shape[1]
    tiles = hidden // TILE
    middle = rows // 2
    near = near_first(deep)
    zs = [z] + [pick([near[i][k] for i in range(deep)], z) for k in range(1, deep)]

    def at(kind, k):
        dx, dy = {"col": (0, 0), "dx": (1, 0), "dy": (0, 1), "diag": (1, 1)}[kind]
        return zs[k] * 2 + (1 - y if dy else y), (1 - x if dx else x)

    def copy(spot, a, way, part=None):
        p, xx = spot
        if part is None:
            rng = pl.ds(core * rows, rows)
        else:
            rng = pl.ds(core * rows + part * middle, middle)
        ref = land.at[p, xx, a, rng, :]
        who = 1 if way == SIBLING else 0
        arrive = half.at[p, a] if part == 1 else recv.at[who, p, xx, a]
        return pltpu.make_async_remote_copy(
            src_ref=ref, dst_ref=ref, send_sem=send.at[way, p, xx, a], recv_sem=arrive,
            device_id=here.device(way), device_id_type=MESH)

    def wait_in(spot, a, part=None):
        copy(spot, a, ACROSS_X, part).wait_recv()

    def wait_sibling(spot, a):
        p, xx = spot
        ref = land.at[p, xx, a, pl.ds((1 - core) * rows, rows), :]
        pltpu.make_async_remote_copy(
            src_ref=ref, dst_ref=ref, send_sem=send.at[SIBLING, p, xx, a], recv_sem=recv.at[1, p, xx, a],
            device_id=here.device(SIBLING), device_id_type=MESH).wait_recv()

    waits = []

    def start(spot, a, way, part=None, when=None):
        def go():
            copy(spot, a, way, part).start()

        def done():
            copy(spot, a, way, part).wait_send()

        if when is None:
            go()
        else:
            pl.when(when)(go)
        waits.append((done, when))

    def along_z(spot, a, k):
        can_up, can_down = z < deep - 1, z > 0
        if k > 0:
            can_up = jnp.logical_and(can_up, zs[k] < z)
            can_down = jnp.logical_and(can_down, zs[k] > z)
        start(spot, a, UP, when=can_up)
        start(spot, a, DOWN, when=can_down)

    def spread(k, a):
        spot = at("col", k)
        along_z(spot, a, k)
        start(spot, a, ACROSS_X)
        start(spot, a, ACROSS_Y)
        start(spot, a, SIBLING)

    def col(k, a):
        wait_in(at("col", k), a)
        spread(k, a)

    def dx(k, a):
        spot = at("dx", k)
        wait_in(spot, a)
        if a == 1 or k == 0:
            start(spot, a, ACROSS_Y, part=1)
        start(spot, a, SIBLING)

    def dy(k, a):
        spot = at("dy", k)
        wait_in(spot, a)
        if a == 1 or k == 0:
            start(spot, a, ACROSS_X, part=0)
        start(spot, a, SIBLING)

    def diag(k, a):
        spot = at("diag", k)
        if a == 1 or k == 0:
            wait_in(spot, a, part=0)
            wait_in(spot, a, part=1)
        else:
            wait_in(spot, a)
        if a == 0:
            along_z(spot, a, k)
        start(spot, a, SIBLING)

    order = [("col", 0), ("col", 1), ("dx", 0), ("dy", 0), ("diag", 0), ("col", 2), ("dx", 1), ("dy", 1),
             ("col", 3), ("diag", 1), ("dx", 2), ("dy", 2), ("diag", 2), ("dx", 3), ("dy", 3), ("diag", 3)]
    events = {
        0: [(col, 1, 0), (dx, 0, 0), (dy, 0, 0), (col, 1, 1), (dx, 0, 1), (dy, 0, 1)],
        2: [(diag, 0, 0), (diag, 0, 1), (col, 2, 0)],
        3: [(col, 2, 1), (dx, 1, 0), (dy, 1, 0)],
        5: [(dx, 1, 1), (dy, 1, 1), (col, 3, 0)],
        6: [(col, 3, 1), (diag, 1, 0), (diag, 1, 1)],
        8: [(dx, 2, 0), (dy, 2, 0)],
        9: [(dx, 2, 1), (dy, 2, 1), (diag, 2, 0), (diag, 2, 1)],
        11: [(dx, 3, 0), (dy, 3, 0), (dx, 3, 1), (dy, 3, 1)],
        13: [(diag, 3, 0), (diag, 3, 1)],
    }

    def load(i):
        p, _ = at(*order[i])
        band = pl.ds(p * width, width)
        slot = i % 2
        return [
            pltpu.make_async_copy(wg_ref.at[band, :], weights_a.at[slot, 0], weight_sems.at[slot, 0]),
            pltpu.make_async_copy(wu_ref.at[band, :], weights_a.at[slot, 1], weight_sems.at[slot, 1]),
            pltpu.make_async_copy(wd_ref.at[:, band], weights_d.at[slot], weight_sems.at[slot, 2]),
        ]

    own = at("col", 0)
    mine = pl.ds(core * rows, rows)
    fetch = [
        pltpu.make_async_copy(x_ref, land.at[own[0], own[1], 0, mine, :], own_sems.at[0]),
        pltpu.make_async_copy(g_ref, land.at[own[0], own[1], 1, mine, :], own_sems.at[1]),
    ]
    for c in fetch:
        c.start()
    for i in (0, 1):
        for c in load(i):
            c.start()
    here.greet()
    for c in fetch:
        c.wait()

    shares = []
    for i, way in enumerate((SIBLING, ACROSS_X, ACROSS_BOTH)):
        shares.append(pltpu.make_async_remote_copy(
            src_ref=s_ref, dst_ref=share_land.at[i], send_sem=share_sems.at[0, i],
            recv_sem=share_sems.at[1, i], device_id=here.device(way), device_id_type=MESH))
        shares[-1].start()
    spread(0, 0)
    spread(0, 1)

    seen = set()
    for i, (kind, k) in enumerate(order):
        spot = at(kind, k)
        xx = spot[1]
        wait_sibling(spot, 0)
        wait_sibling(spot, 1)
        for c in load(i):
            c.wait()
        slot = i % 2
        side = kind in ("dx", "diag")
        first = side not in seen
        seen.add(side)

        def tile(n, carry, spot=spot, slot=slot, first=first, xx=xx):
            cols = pl.ds(pl.multiple_of(n * TILE, TILE), TILE)
            inputs, grads = land[spot[0], spot[1], 0], land[spot[0], spot[1], 1]
            gate = jnp.dot(inputs, weights_a[slot, 0, :, cols], preferred_element_type=jnp.float32)
            up = jnp.dot(inputs, weights_a[slot, 1, :, cols], preferred_element_type=jnp.float32)
            back = lax.dot_general(grads, weights_d[slot, cols, :], NT, preferred_element_type=jnp.float32)
            if first:
                acc[0, xx, n], acc[1, xx, n], acc[2, xx, n] = gate, up, back
            else:
                acc[0, xx, n] += gate
                acc[1, xx, n] += up
                acc[2, xx, n] += back
            return carry

        lax.fori_loop(0, tiles, tile, 0)
        if i + 2 < len(order):
            for c in load(i + 2):
                c.start()
        for event, kk, a in events.get(i, []):
            event(kk, a)

        def finish(xx):
            def body(n, carry):
                cols = pl.ds(pl.multiple_of(n * TILE, TILE), TILE)
                gate, up, back = acc[0, xx, n], acc[1, xx, n], acc[2, xx, n]
                sigma = 1.0 / (1.0 + jnp.exp(-gate))
                scaled = back * sigma
                later = pl.ds(pl.multiple_of(hidden + n * TILE, TILE), TILE)
                stage[xx, :, cols] = (scaled * up * (1.0 + gate * (1.0 - sigma))).astype(jnp.bfloat16)
                stage[xx, :, later] = (scaled * gate).astype(jnp.bfloat16)
                return carry

            lax.fori_loop(0, tiles, body, 0)
            pltpu.make_async_copy(stage.at[xx], act_ref.at[xx], out_sems.at[xx]).start()

        if i == len(order) - 2:
            finish(x)
        if i == len(order) - 1:
            finish(1 - x)
    share_ref[here.ep] = s_ref[...]
    for i, way in enumerate((SIBLING, ACROSS_X, ACROSS_BOTH)):
        shares[i].wait()
        share_ref[here.device(way)[0]] = share_land[i]
    for xx in (x, 1 - x):
        pltpu.make_async_copy(stage.at[xx], act_ref.at[xx], out_sems.at[xx]).wait()
    for done, when in waits:
        if when is None:
            done()
        else:
            pl.when(when)(done)


DIAG, DY, DX, OWN = range(4)
HALF_X, HALF_Y, WHOLE_Y, WHOLE_X, ALONG_Z = range(4, 9)


def scatter_kernel(deep, act_ref, share_ref, wg_ref, wu_ref, out_ref,
                   acts, weights, share_cols, own, sib_out, sib_in, blocks, in_half, in_x, in_y, in_z,
                   send, recv, recv_z, act_sems, weight_sems):
    here = Place(deep)
    x, y, z, core = here.x, here.y, here.z, here.core
    rows, width = out_ref.shape
    hidden = wg_ref.shape[1]
    middle = rows // 2
    far = [line[::-1] for line in near_first(deep)]
    dest = [pick([far[i][k] for i in range(deep)], z) for k in range(deep - 1)] + [z]

    def load(pair):
        k, same = pair // 2, pair % 2
        band = pl.ds((dest[k] * 2 + (y if same else 1 - y)) * width, width)
        slot = pair % 2
        return [
            pltpu.make_async_copy(wg_ref.at[band, :], weights.at[slot, :, pl.ds(0, hidden)], weight_sems.at[slot, 0]),
            pltpu.make_async_copy(wu_ref.at[band, :], weights.at[slot, :, pl.ds(hidden, hidden)], weight_sems.at[slot, 1]),
        ]

    fetch = [pltpu.make_async_copy(act_ref.at[xx], acts.at[xx], act_sems.at[xx]) for xx in (1 - x, x)]
    fetch[0].start()
    for c in load(0):
        c.start()
    fetch[1].start()
    for c in load(1):
        c.start()
    for b in range(share_ref.shape[0]):
        table = share_ref[b].T
        chosen = lax.broadcasted_iota(jnp.int32, table.shape, 1) == here.ep
        column = jnp.sum(jnp.where(chosen, table, 0.0), axis=1, keepdims=True)
        share_cols[b] = jnp.broadcast_to(column, share_cols.shape[1:])
    here.greet()

    waits = []

    def remote(src, dst, kind, k, way, arrive=None):
        return pltpu.make_async_remote_copy(
            src_ref=src, dst_ref=dst, send_sem=send.at[kind, k],
            recv_sem=recv.at[kind, k] if arrive is None else arrive,
            device_id=here.device(way), device_id_type=MESH)

    low, high = pl.ds(0, middle), pl.ds(middle, middle)

    def sib(kind, k):
        return remote(sib_out.at[kind, k], sib_in.at[kind, k], kind, k, SIBLING)

    def half_x(k):
        return remote(blocks.at[DIAG, k, low], in_half.at[k, low], HALF_X, k, ACROSS_X)

    def half_y(k):
        return remote(blocks.at[DIAG, k, high], in_half.at[k, high], HALF_Y, k, ACROSS_Y)

    def whole_y(k):
        return remote(blocks.at[DY, k], in_y.at[k], WHOLE_Y, k, ACROSS_Y)

    def whole_x(k):
        return remote(blocks.at[DX, k], in_x.at[k], WHOLE_X, k, ACROSS_X)

    def line_up(k):
        return remote(blocks.at[OWN, k], in_z.at[0, dest[k]], ALONG_Z, k, UP, recv_z.at[0, dest[k]])

    def line_down(k):
        return remote(blocks.at[OWN, k], in_z.at[1, dest[k]], ALONG_Z, k, DOWN, recv_z.at[1, dest[k]])

    def begin(make, k, when=None):
        if when is None:
            make(k).start()
        else:
            pl.when(when)(lambda: make(k).start())
        waits.append((make, k, when))

    def half_of(t, part):
        kind, k = t % 4, t // 4
        xx = x if kind in (DY, OWN) else 1 - x
        slot = (t // 2) % 2
        block = 1 - core if part == 0 else core
        value = lax.dot_general(
            acts[xx, pl.ds(block * rows, rows), :], weights[slot], NT, preferred_element_type=jnp.float32)
        value = value * share_cols[xx * CORES + block][:, :1]
        if part == 0:
            sib_out[kind, k] = value.astype(jnp.bfloat16)
            begin(lambda k: sib(kind, k), k)
        else:
            own[kind, k] = value

    def c_diag(k):
        sib(DIAG, k).wait_recv()
        blocks[DIAG, k] = (own[DIAG, k] + sib_in[DIAG, k].astype(jnp.float32)).astype(jnp.bfloat16)
        begin(half_x, k)
        begin(half_y, k)

    def c_side(k, kind, arrived, part, whole):
        sib(kind, k).wait_recv()
        arrived(k).wait_recv()
        other = pl.ds(middle - part.start, middle)
        blocks[kind, k, other] = (
            own[kind, k, other] + sib_in[kind, k, other].astype(jnp.float32)).astype(jnp.bfloat16)
        blocks[kind, k, part] = (
            own[kind, k, part] + sib_in[kind, k, part].astype(jnp.float32)
            + in_half[k, part].astype(jnp.float32)).astype(jnp.bfloat16)
        begin(whole, k)

    def c_dy(k):
        c_side(k, DY, half_x, low, whole_y)

    def c_dx(k):
        c_side(k, DX, half_y, high, whole_x)

    def up_in(k):
        return jnp.logical_and(dest[k] > z, z > 0)

    def down_in(k):
        return jnp.logical_and(dest[k] < z, z < deep - 1)

    def pass_on(k, when):
        begin(line_up, k, jnp.logical_and(when, dest[k] > z))
        begin(line_down, k, jnp.logical_and(when, dest[k] < z))

    def c_own(k):
        sib(OWN, k).wait_recv()
        whole_x(k).wait_recv()
        whole_y(k).wait_recv()
        own[OWN, k] = (own[OWN, k] + sib_in[OWN, k].astype(jnp.float32)
                       + (in_x[k].astype(jnp.float32) + in_y[k].astype(jnp.float32)))
        if k < deep - 1:
            blocks[OWN, k] = own[OWN, k].astype(jnp.bfloat16)
            pass_on(k, jnp.logical_not(jnp.logical_or(up_in(k), down_in(k))))

    def chain(k):
        def add(make, side):
            make(k).wait_recv()
            blocks[OWN, k] = (own[OWN, k] + in_z[side, dest[k]].astype(jnp.float32)).astype(jnp.bfloat16)

        pl.when(up_in(k))(lambda: add(line_up, 0))
        pl.when(down_in(k))(lambda: add(line_down, 1))
        pass_on(k, jnp.logical_or(up_in(k), down_in(k)))

    during, after = {}, {}
    for k in range(deep):
        during.setdefault(4 * k + 1, []).append((c_diag, k))
        during.setdefault(4 * k + 3, []).append((c_dy, k))
        after.setdefault(4 * k + 3, []).append((c_dx, k))
        if k < deep - 2:
            during.setdefault(4 * k + 7, []).append((c_own, k))
            during.setdefault(4 * k + 11, []).append((chain, k))

    units = 4 * deep
    fetch[0].wait()
    for t in range(units):
        if t == 1:
            fetch[1].wait()
        if t % 2 == 0:
            for c in load(t // 2):
                c.wait()
        half_of(t, 0)
        for task, k in during.get(t, []):
            task(k)
        half_of(t, 1)
        if t % 2 == 1 and t // 2 + 2 < units // 2:
            for c in load(t // 2 + 2):
                c.start()
        for task, k in after.get(t, []):
            task(k)
    for k in range(max(deep - 2, 0), deep - 1):
        c_own(k)
    for k in range(max(deep - 2, 0), deep - 1):
        chain(k)
    last = deep - 1
    c_own(last)

    def add_line(make, side):
        make(last).wait_recv()
        own[OWN, last] += in_z[side, z].astype(jnp.float32)

    pl.when(z > 0)(lambda: add_line(line_up, 0))
    pl.when(z < deep - 1)(lambda: add_line(line_down, 1))
    out_ref[...] = own[OWN, last].astype(out_ref.dtype)
    for make, k, when in waits:
        if when is None:
            make(k).wait_send()
        else:
            pl.when(when)(lambda: make(k).wait_send())


def kernels(layer_input, out_grad, route, gate_share, gate_weight, up_weight, down_weight):
    groups, members = lax.axis_size("ep"), lax.axis_size("tp")
    deep = members // 2
    rows, width = layer_input.shape
    hidden = gate_weight.shape[2]
    tiles = hidden // TILE
    chips = groups // CORES
    experts = jnp.arange(8, dtype=jnp.int32)
    shares = jnp.sum(
        jnp.where(route.T[None, :, :] == experts[:, None, None], gate_share.T[None, :, :], 0.0), axis=1)
    gate_matrix, up_matrix, down_matrix = gate_weight[0], up_weight[0], down_weight[0]
    anywhere = pl.BlockSpec(memory_space=pl.ANY)
    local = pl.BlockSpec(memory_space=pltpu.VMEM)
    bf16, f32 = jnp.bfloat16, jnp.float32
    both = CORES * rows
    dma = pltpu.SemaphoreType.DMA
    acts, shares = pl.pallas_call(
        functools.partial(gather_kernel, deep),
        out_shape=(
            jax.ShapeDtypeStruct((chips, both, 2 * hidden), bf16),
            jax.ShapeDtypeStruct((groups, 8, rows), f32),
        ),
        in_specs=[anywhere, anywhere, local, anywhere, anywhere, anywhere],
        out_specs=(anywhere, local),
        scratch_shapes=[
            pltpu.VMEM((members, chips, 2, both, width), bf16),
            pltpu.VMEM((3, 8, rows), f32),
            pltpu.VMEM((3, chips, tiles, both, TILE), f32),
            pltpu.VMEM((2, 2, width, hidden), bf16),
            pltpu.VMEM((2, hidden, width), bf16),
            pltpu.VMEM((chips, both, 2 * hidden), bf16),
            dma((5, members, chips, 2)),
            dma((2, members, chips, 2)),
            dma((members, 2)),
            dma((2, 3)),
            dma((2,)),
            dma((2, 3)),
            dma((chips,)),
        ],
        compiler_params=pltpu.CompilerParams(
            collective_id=0, has_side_effects=True, vmem_limit_bytes=VMEM_BYTES),
        name="gather",
    )(layer_input, out_grad, shares, gate_matrix, up_matrix, down_matrix)
    return pl.pallas_call(
        functools.partial(scatter_kernel, deep),
        out_shape=jax.ShapeDtypeStruct((rows, width), bf16),
        in_specs=[anywhere, local, anywhere, anywhere],
        out_specs=local,
        scratch_shapes=[
            pltpu.VMEM((chips, both, 2 * hidden), bf16),
            pltpu.VMEM((2, width, 2 * hidden), bf16),
            pltpu.VMEM((groups, rows, 128), f32),
            pltpu.VMEM((4, deep, rows, width), f32),
            pltpu.VMEM((4, deep, rows, width), bf16),
            pltpu.VMEM((4, deep, rows, width), bf16),
            pltpu.VMEM((4, deep, rows, width), bf16),
            pltpu.VMEM((deep, rows, width), bf16),
            pltpu.VMEM((deep, rows, width), bf16),
            pltpu.VMEM((deep, rows, width), bf16),
            pltpu.VMEM((2, deep, rows, width), bf16),
            dma((9, deep)),
            dma((8, deep)),
            dma((2, deep)),
            dma((chips,)),
            dma((2, 2)),
        ],
        compiler_params=pltpu.CompilerParams(
            collective_id=1, has_side_effects=True, vmem_limit_bytes=VMEM_BYTES),
        name="scatter",
    )(acts, shares, gate_matrix, up_matrix)


def permutes(layer_input, out_grad, route, gate_share, gate_weight, up_weight, down_weight):
    groups = lax.axis_size("ep")
    me = lax.axis_index("ep")
    chips = groups // CORES
    rows = layer_input.shape[0]
    gate_matrix = gate_weight[0]
    up_matrix = up_weight[0]
    down_matrix = down_weight[0]

    def shift(value, step):
        pairs = [(i, (i + step * CORES) % groups) for i in range(groups)]
        return lax.ppermute(value, "ep", pairs)

    def swap(value):
        return lax.ppermute(value, "ep", [(i, i ^ 1) for i in range(groups)])

    members = lax.axis_size("tp")
    inner = 1
    while 4 * inner * inner <= members:
        inner *= 2
    outer = members // inner
    place = lax.axis_index("tp")
    place_outer, place_inner = place // inner, place % inner
    width = layer_input.shape[1]

    def turn(value, outer_step, inner_step):
        pairs = []
        for i in range(members):
            target = (i // inner + outer_step) % outer * inner + (i % inner + inner_step) % inner
            pairs.append((i, target))
        return lax.ppermute(value, "tp", pairs)

    def gather(value):
        line = jnp.stack([value] + [turn(value, a, 0) for a in range(1, outer)])
        return jnp.concatenate([line] + [turn(line, 0, b) for b in range(1, inner)])

    def in_order(blocks):
        both = jnp.concatenate([blocks, swap(blocks)], axis=1)
        full = jnp.zeros((both.shape[1], members * width), both.dtype)
        for b in range(inner):
            for a in range(outer):
                source = (place_outer - a) % outer * inner + (place_inner - b) % inner
                full = lax.dynamic_update_slice(full, both[b * outer + a], (0, source * width))
        return full

    def scatter(value):
        def blocks_for(b):
            owner = (place_inner + b) % inner
            return [
                lax.dynamic_slice_in_dim(
                    value, ((place_outer + a) % outer * inner + owner) * width, width, axis=1
                )
                for a in range(outer)
            ]

        lines = jnp.stack(blocks_for(0))
        for b in range(1, inner):
            sent = jnp.stack(blocks_for(b)).astype(jnp.bfloat16)
            lines = lines + turn(sent, 0, b).astype(jnp.float32)
        result = lines[0]
        for a in range(1, outer):
            sent = turn(lines[a].astype(jnp.bfloat16), a, 0)
            result = result + sent.astype(jnp.float32)
        return result

    experts = jnp.arange(groups, dtype=jnp.int32)
    shares = jnp.sum(
        jnp.where(route[:, :, None] == experts, gate_share[:, :, None], 0.0), axis=1
    )

    gathered = []
    for step in range(chips):
        if step:
            part_input, part_grad = shift(layer_input, step), shift(out_grad, step)
            part_share = shift(shares, step)
        else:
            part_input, part_grad, part_share = layer_input, out_grad, shares
        full_input = gather(part_input)
        full_grad = gather(part_grad)
        share = jnp.concatenate([part_share, swap(part_share)], axis=0)
        share = jnp.sum(jnp.where(experts == me, share, 0.0), axis=1, keepdims=True)
        gathered.append((full_input, full_grad, share))

    total = None
    for step in range(chips):
        full_input, full_grad, share = gathered[step]
        inputs = in_order(full_input)
        grads = in_order(full_grad)
        gate_sum = jnp.dot(inputs, gate_matrix, preferred_element_type=jnp.float32)
        up_sum = jnp.dot(inputs, up_matrix, preferred_element_type=jnp.float32)
        hidden_sum = lax.dot_general(
            grads, down_matrix, (((1,), (1,)), ((), ())), preferred_element_type=jnp.float32
        )
        sigma = jax.nn.sigmoid(gate_sum)
        slope = sigma * (1.0 + gate_sum * (1.0 - sigma))
        gate_grad = (hidden_sum * up_sum * slope).astype(jnp.bfloat16)
        up_grad = (hidden_sum * gate_sum * sigma).astype(jnp.bfloat16)
        partial = lax.dot_general(
            gate_grad, gate_matrix, (((1,), (1,)), ((), ())), preferred_element_type=jnp.float32
        )
        partial = partial + lax.dot_general(
            up_grad, up_matrix, (((1,), (1,)), ((), ())), preferred_element_type=jnp.float32
        )
        partial = jnp.where(share > 0.0, partial * share, 0.0)
        other = swap(partial[rows:].astype(jnp.bfloat16))
        summed = scatter(partial[:rows] + other.astype(jnp.float32))
        if step:
            summed = shift(summed.astype(jnp.bfloat16), chips - step).astype(jnp.float32)
        total = summed if total is None else total + summed
    return total.astype(jnp.bfloat16)


def solution(mesh):
    groups, members = mesh.shape["ep"], mesh.shape["tp"]
    fits = groups == 2 * CORES and members == 8
    return jax.shard_map(
        kernels if fits else permutes,
        mesh=mesh,
        in_specs=(
            P("ep", "tp"),
            P("ep", "tp"),
            P("ep", None),
            P("ep", None),
            P("ep", None, "tp"),
            P("ep", None, "tp"),
            P("ep", "tp", None),
        ),
        out_specs=P("ep", "tp"),
        check_vma=False,
    )
```

```python
import functools

import jax
import jax.numpy as jnp
from jax import lax
from jax.experimental import pallas as pl
from jax.experimental.pallas import tpu as pltpu
from jax.sharding import PartitionSpec as P

CORES = 2
TILE = 256
VMEM_BYTES = 67_043_328
NT = (((1,), (1,)), ((), ()))
MESH = pl.DeviceIdType.MESH
UP, DOWN, ACROSS_X, ACROSS_Y, SIBLING, ACROSS_BOTH = range(6)


def pick(table, index):
    value = jnp.int32(table[-1])
    for i in range(len(table) - 1):
        value = jnp.where(index == i, jnp.int32(table[i]), value)
    return value


class Place:
    def __init__(self, deep):
        ep, tp = lax.axis_index("ep"), lax.axis_index("tp")
        self.deep = deep
        self.x, self.core = ep // CORES, ep % CORES
        self.z, self.y = tp // 2, tp % 2
        self.ep, self.tp = ep, tp

    def device(self, way):
        ep, tp = self.ep, self.tp
        if way == SIBLING:
            return (self.x * CORES + 1 - self.core, tp)
        if way == ACROSS_X:
            return ((1 - self.x) * CORES + self.core, tp)
        if way == ACROSS_BOTH:
            return ((1 - self.x) * CORES + 1 - self.core, tp)
        if way == ACROSS_Y:
            return (ep, self.z * 2 + 1 - self.y)
        return (ep, tp + 2 if way == UP else tp - 2)

    def greet(self):
        barrier = pltpu.get_barrier_semaphore()

        def signal(way):
            pl.semaphore_signal(barrier, inc=1, device_id=self.device(way), device_id_type=MESH)

        ways = (SIBLING, ACROSS_X, ACROSS_Y, ACROSS_BOTH)
        for way in ways:
            signal(way)
        pl.when(self.z < self.deep - 1)(lambda: signal(UP))
        pl.when(self.z > 0)(lambda: signal(DOWN))
        lines = (self.z > 0).astype(jnp.int32) + (self.z < self.deep - 1).astype(jnp.int32)
        pl.semaphore_wait(barrier, len(ways) + lines)


def near_first(deep):
    return [sorted(range(deep), key=lambda other: (abs(other - z), other)) for z in range(deep)]


def gather_kernel(deep, x_ref, g_ref, s_ref, wg_ref, wu_ref, wd_ref, act_ref, share_ref,
                  land, share_land, acc, weights_a, weights_d, stage,
                  send, recv, half, share_sems, own_sems, weight_sems, out_sems):
    here = Place(deep)
    x, y, z, core = here.x, here.y, here.z, here.core
    rows, width = x_ref.shape
    hidden = wg_ref.shape[1]
    tiles = hidden // TILE
    middle = rows // 2
    near = near_first(deep)
    zs = [z] + [pick([near[i][k] for i in range(deep)], z) for k in range(1, deep)]

    def at(kind, k):
        dx, dy = {"col": (0, 0), "dx": (1, 0), "dy": (0, 1), "diag": (1, 1)}[kind]
        return zs[k] * 2 + (1 - y if dy else y), (1 - x if dx else x)

    def copy(spot, a, way, part=None):
        p, xx = spot
        if part is None:
            rng = pl.ds(core * rows, rows)
        else:
            rng = pl.ds(core * rows + part * middle, middle)
        ref = land.at[p, xx, a, rng, :]
        who = 1 if way == SIBLING else 0
        arrive = half.at[p, a] if part == 1 else recv.at[who, p, xx, a]
        return pltpu.make_async_remote_copy(
            src_ref=ref, dst_ref=ref, send_sem=send.at[way, p, xx, a], recv_sem=arrive,
            device_id=here.device(way), device_id_type=MESH)

    def wait_in(spot, a, part=None):
        copy(spot, a, ACROSS_X, part).wait_recv()

    def wait_sibling(spot, a):
        p, xx = spot
        ref = land.at[p, xx, a, pl.ds((1 - core) * rows, rows), :]
        pltpu.make_async_remote_copy(
            src_ref=ref, dst_ref=ref, send_sem=send.at[SIBLING, p, xx, a], recv_sem=recv.at[1, p, xx, a],
            device_id=here.device(SIBLING), device_id_type=MESH).wait_recv()

    inner = jnp.logical_and(z > 0, z < deep - 1)
    outer = jnp.logical_not(inner)
    sent = []

    def guarded(k, side, way, go):
        conds = {"all": [], "inner": [inner], "outer": [outer]}[side]
        if way == UP:
            conds = conds + [z < deep - 1] + ([zs[k] < z] if k else [])
        if way == DOWN:
            conds = conds + [z > 0] + ([zs[k] > z] if k else [])
        if conds:
            pl.when(functools.reduce(jnp.logical_and, conds))(go)
        else:
            go()

    def start(kind, k, a, way, side, part=None):
        sent.append((kind, k, a, way, side, part))
        guarded(k, side, way, lambda: copy(at(kind, k), a, way, part).start())

    def finish_sends():
        for kind, k, a, way, side, part in dict.fromkeys(sent):
            guarded(k, side, way, lambda: copy(at(kind, k), a, way, part).wait_send())

    def col(k, a, side="all"):
        if k > 0:
            guarded(k, side, None, lambda: wait_in(at("col", k), a))
        start("col", k, a, UP, side)
        start("col", k, a, DOWN, side)
        start("col", k, a, SIBLING, side)

    def cross(k, a, side="all"):
        start("col", k, a, ACROSS_X, side)
        start("col", k, a, ACROSS_Y, side)

    def dx(k, a, side="all"):
        wait_in(at("dx", k), a)
        if a == 1 or k == 0:
            start("dx", k, a, ACROSS_Y, side, part=1)
        start("dx", k, a, SIBLING, side)

    def dy(k, a, side="all"):
        wait_in(at("dy", k), a)
        if a == 1 or k == 0:
            start("dy", k, a, ACROSS_X, side, part=0)
        start("dy", k, a, SIBLING, side)

    def diag(k, a, side="all"):
        split = a == 1 or k == 0

        def arrived():
            wait_in(at("diag", k), a, part=0 if split else None)
            if split:
                wait_in(at("diag", k), a, part=1)

        guarded(k, side, None, arrived)
        if a == 0:
            start("diag", k, a, UP, side)
            start("diag", k, a, DOWN, side)
        start("diag", k, a, SIBLING, side)

    order = [("col", 0), ("col", 1), ("dx", 0), ("dy", 0), ("col", 2), ("diag", 0), ("dx", 1), ("dy", 1),
             ("col", 3), ("diag", 1), ("dx", 2), ("dy", 2), ("diag", 2), ("dx", 3), ("dy", 3), ("diag", 3)]
    count = len(order)

    def near_pair(a):
        return [(col, 1, a, "all"), (col, 2, a, "inner"), (dx, 0, a, "all"), (dy, 0, a, "all"),
                (cross, 1, a, "all"), (cross, 2, a, "inner")]

    def far_col(k, a, cond):
        return [(col, k, a, cond), (cross, k, a, cond)]

    events = {
        0: near_pair(0) + near_pair(1),
        1: [(diag, 0, 0, "all")] + far_col(2, 0, "outer") + far_col(3, 0, "inner"),
        3: [(dx, 1, 0, "all"), (dy, 1, 0, "all")] + far_col(2, 1, "outer") + far_col(3, 1, "inner"),
        4: [(diag, 0, 1, "all")],
        5: [(dx, 1, 1, "all"), (dy, 1, 1, "all")],
        6: far_col(3, 0, "outer"),
        7: far_col(3, 1, "outer") + [(diag, 1, 0, "all"), (diag, 2, 0, "inner"), (diag, 1, 1, "all"),
                                   (dx, 2, 0, "all"), (dy, 2, 0, "all")],
        8: [(dx, 2, 1, "all"), (dy, 2, 1, "all")],
        9: [(diag, 2, 0, "outer"), (diag, 3, 0, "inner"), (diag, 2, 1, "all")],
        10: [(dx, 3, 0, "all"), (dy, 3, 0, "all")],
        11: [(dx, 3, 1, "all"), (dy, 3, 1, "all")],
        12: [(diag, 3, 0, "outer"), (diag, 3, 1, "all")],
    }

    def spot_of(i):
        plane = zs[-1]
        step = pick([k for _, k in order], i)
        for k in range(deep - 1):
            plane = jnp.where(step == k, zs[k], plane)
        turned_x = pick([int(kind in ("dx", "diag")) for kind, _ in order], i)
        turned_y = pick([int(kind in ("dy", "diag")) for kind, _ in order], i)
        return plane * 2 + (y + turned_y) % 2, (x + turned_x) % 2

    def load(i):
        p, _ = spot_of(i)
        band = pl.ds(p * width, width)
        slot = i % 2
        return [
            pltpu.make_async_copy(wg_ref.at[band, :], weights_a.at[slot, 0], weight_sems.at[slot, 0]),
            pltpu.make_async_copy(wu_ref.at[band, :], weights_a.at[slot, 1], weight_sems.at[slot, 1]),
            pltpu.make_async_copy(wd_ref.at[:, band], weights_d.at[slot], weight_sems.at[slot, 2]),
        ]

    own = at("col", 0)
    mine = pl.ds(core * rows, rows)
    fetch = [
        pltpu.make_async_copy(x_ref, land.at[own[0], own[1], 0, mine, :], own_sems.at[0]),
        pltpu.make_async_copy(g_ref, land.at[own[0], own[1], 1, mine, :], own_sems.at[1]),
    ]
    for c in fetch:
        c.start()
    for i in (0, 1):
        for c in load(jnp.int32(i)):
            c.start()
    here.greet()
    for c in fetch:
        c.wait()

    shares = []
    for i, way in enumerate((SIBLING, ACROSS_X, ACROSS_BOTH)):
        shares.append(pltpu.make_async_remote_copy(
            src_ref=s_ref, dst_ref=share_land.at[i], send_sem=share_sems.at[0, i],
            recv_sem=share_sems.at[1, i], device_id=here.device(way), device_id_type=MESH))
        shares[-1].start()
    for a in (0, 1):
        col(0, a)
        cross(0, a)

    def clear(n, carry):
        for xx in range(acc.shape[1]):
            for j in range(3):
                acc[j, xx, n] = jnp.zeros(acc.shape[3:], acc.dtype)
        return carry

    lax.fori_loop(0, tiles, clear, 0)

    def finish(xx):
        def body(n, carry):
            cols = pl.ds(pl.multiple_of(n * TILE, TILE), TILE)
            later = pl.ds(pl.multiple_of(hidden + n * TILE, TILE), TILE)
            gate, up, back = acc[0, xx, n], acc[1, xx, n], acc[2, xx, n]
            sigma = 0.5 * jnp.tanh(0.5 * gate) + 0.5
            scaled = back * sigma
            stage[xx, :, cols] = (scaled * up * (1.0 + gate * (1.0 - sigma))).astype(jnp.bfloat16)
            stage[xx, :, later] = (scaled * gate).astype(jnp.bfloat16)
            return carry

        lax.fori_loop(0, tiles, body, 0)
        pltpu.make_async_copy(stage.at[xx], act_ref.at[xx], out_sems.at[xx]).start()

    def unit(i, carry):
        p, xx = spot_of(i)
        slot = i % 2
        wait_sibling((p, xx), 0)
        wait_sibling((p, xx), 1)
        for c in load(i):
            c.wait()
        for n in range(tiles):
            cols = pl.ds(n * TILE, TILE)
            acc[0, xx, n] += jnp.dot(
                land[p, xx, 0], weights_a[slot, 0, :, cols], preferred_element_type=jnp.float32)
            acc[1, xx, n] += jnp.dot(
                land[p, xx, 0], weights_a[slot, 1, :, cols], preferred_element_type=jnp.float32)
            acc[2, xx, n] += lax.dot_general(
                land[p, xx, 1], weights_d[slot, cols, :], NT, preferred_element_type=jnp.float32)

        @pl.when(i + 2 < count)
        def _():
            for c in load(i + 2):
                c.start()

        for when, tasks in events.items():
            @pl.when(i == when)
            def _(tasks=tasks):
                for task, k, a, cond in tasks:
                    task(k, a, cond)

        pl.when(i == count - 2)(lambda: finish(x))
        pl.when(i == count - 1)(lambda: finish(1 - x))
        return carry

    lax.fori_loop(0, count, unit, 0)
    share_ref[here.ep] = s_ref[...]
    for i, way in enumerate((SIBLING, ACROSS_X, ACROSS_BOTH)):
        shares[i].wait()
        share_ref[here.device(way)[0]] = share_land[i]
    for xx in (x, 1 - x):
        pltpu.make_async_copy(stage.at[xx], act_ref.at[xx], out_sems.at[xx]).wait()
    finish_sends()


DIAG, DY, DX, OWN = range(4)
HALF_X, HALF_Y, WHOLE_Y, WHOLE_X, ALONG_Z = range(4, 9)


def scatter_kernel(deep, act_ref, share_ref, wg_ref, wu_ref, out_ref,
                   acts, weights, share_cols, own, sib_out, sib_in, blocks, in_half, in_x, in_y, in_z,
                   send, recv, recv_z, act_sems, weight_sems):
    here = Place(deep)
    x, y, z, core = here.x, here.y, here.z, here.core
    rows, width = out_ref.shape
    hidden = wg_ref.shape[1]
    middle = rows // 2
    far = [line[::-1] for line in near_first(deep)]
    dests = [pick([far[i][k] for i in range(deep)], z) for k in range(deep - 1)] + [z]

    def dest(k):
        value = dests[-1]
        for j in range(deep - 1):
            value = jnp.where(k == j, dests[j], value)
        return value

    def load(k, same):
        band = pl.ds((dest(k) * 2 + (y if same else 1 - y)) * width, width)
        return [
            pltpu.make_async_copy(
                ref.at[band, :], weights.at[same, :, pl.ds(j * hidden, hidden)], weight_sems.at[same, j])
            for j, ref in enumerate((wg_ref, wu_ref))
        ]

    def fetch(xx):
        return [
            pltpu.make_async_copy(
                act_ref.at[xx, pl.ds(block * rows, rows)], acts.at[xx, pl.ds(j * rows, rows)], act_sems.at[xx, j])
            for j, block in enumerate((1 - core, core))
        ]

    first, zero = fetch(1 - x) + load(jnp.int32(0), 0), jnp.int32(0)
    second = fetch(x) + load(zero, 1)
    for c in first:
        c.start()
    for b in range(share_ref.shape[0]):
        table = share_ref[b].T
        chosen = lax.broadcasted_iota(jnp.int32, table.shape, 1) == here.ep
        column = jnp.sum(jnp.where(chosen, table, 0.0), axis=1, keepdims=True)
        share_cols[b] = jnp.broadcast_to(column, share_cols.shape[1:])
    here.greet()
    for c in first:
        c.wait()
    for c in second:
        c.start()

    def remote(src, dst, kind, k, way, arrive=None):
        return pltpu.make_async_remote_copy(
            src_ref=src, dst_ref=dst, send_sem=send.at[kind, k],
            recv_sem=recv.at[kind, k] if arrive is None else arrive,
            device_id=here.device(way), device_id_type=MESH)

    low, high = pl.ds(0, middle), pl.ds(middle, middle)

    def sib(kind, k):
        return remote(sib_out.at[kind, k], sib_in.at[kind, k], kind, k, SIBLING)

    def half_x(k):
        return remote(blocks.at[DIAG, k, low], in_half.at[k, low], HALF_X, k, ACROSS_X)

    def half_y(k):
        return remote(blocks.at[DIAG, k, high], in_half.at[k, high], HALF_Y, k, ACROSS_Y)

    def whole_y(k):
        return remote(blocks.at[DY, k], in_y.at[k], WHOLE_Y, k, ACROSS_Y)

    def whole_x(k):
        return remote(blocks.at[DX, k], in_x.at[k], WHOLE_X, k, ACROSS_X)

    def line_up(k):
        return remote(blocks.at[OWN, k], in_z.at[0, dest(k)], ALONG_Z, k, UP, recv_z.at[0, dest(k)])

    def line_down(k):
        return remote(blocks.at[OWN, k], in_z.at[1, dest(k)], ALONG_Z, k, DOWN, recv_z.at[1, dest(k)])

    def begin(make, k, when=None):
        if when is None:
            make(k).start()
        else:
            pl.when(when)(lambda: make(k).start())

    def multiply(kind, k):
        xx = x if kind in (DY, OWN) else 1 - x
        value = lax.dot_general(
            acts[xx], weights[int(kind in (DX, OWN))], NT, preferred_element_type=jnp.float32)
        other = value[:rows] * share_cols[xx * CORES + 1 - core][:, :1]
        sib_out[kind, k] = other.astype(jnp.bfloat16)
        begin(lambda k: sib(kind, k), k)
        own[kind, k] = value[rows:] * share_cols[xx * CORES + core][:, :1]

    def c_diag(k):
        sib(DIAG, k).wait_recv()
        blocks[DIAG, k] = (own[DIAG, k] + sib_in[DIAG, k].astype(jnp.float32)).astype(jnp.bfloat16)
        begin(half_x, k)
        begin(half_y, k)

    def c_side(k, kind, arrived, part, whole):
        sib(kind, k).wait_recv()
        arrived(k).wait_recv()
        other = pl.ds(middle - part.start, middle)
        blocks[kind, k, other] = (
            own[kind, k, other] + sib_in[kind, k, other].astype(jnp.float32)).astype(jnp.bfloat16)
        blocks[kind, k, part] = (
            own[kind, k, part] + sib_in[kind, k, part].astype(jnp.float32)
            + in_half[k, part].astype(jnp.float32)).astype(jnp.bfloat16)
        begin(whole, k)

    def c_dy(k):
        c_side(k, DY, half_x, low, whole_y)

    def c_dx(k):
        c_side(k, DX, half_y, high, whole_x)

    def up_in(k):
        return jnp.logical_and(dest(k) > z, z > 0)

    def down_in(k):
        return jnp.logical_and(dest(k) < z, z < deep - 1)

    def pass_on(k, when):
        begin(line_up, k, jnp.logical_and(when, dest(k) > z))
        begin(line_down, k, jnp.logical_and(when, dest(k) < z))

    def c_own(k):
        sib(OWN, k).wait_recv()
        whole_x(k).wait_recv()
        whole_y(k).wait_recv()
        own[OWN, k] = (own[OWN, k] + sib_in[OWN, k].astype(jnp.float32)
                       + (in_x[k].astype(jnp.float32) + in_y[k].astype(jnp.float32)))

        @pl.when(k < deep - 1)
        def _():
            blocks[OWN, k] = own[OWN, k].astype(jnp.bfloat16)
            pass_on(k, jnp.logical_not(jnp.logical_or(up_in(k), down_in(k))))

    def chain(k):
        def add(make, side):
            make(k).wait_recv()
            blocks[OWN, k] = (own[OWN, k] + in_z[side, dest(k)].astype(jnp.float32)).astype(jnp.bfloat16)

        pl.when(up_in(k))(lambda: add(line_up, 0))
        pl.when(down_in(k))(lambda: add(line_down, 1))
        pass_on(k, jnp.logical_or(up_in(k), down_in(k)))

    def step(k, carry):
        @pl.when(k > 0)
        def _():
            for c in load(k, 0):
                c.wait()

        multiply(DIAG, k)

        @pl.when(k == 0)
        def _():
            for c in fetch(x):
                c.wait()

        multiply(DY, k)
        c_diag(k)
        for c in load(k, 1):
            c.wait()

        @pl.when(k < deep - 1)
        def _():
            for c in load(k + 1, 0):
                c.start()

        multiply(DX, k)
        multiply(OWN, k)
        c_dy(k)
        c_dx(k)

        @pl.when(k < deep - 1)
        def _():
            for c in load(k + 1, 1):
                c.start()

        pl.when(k > 0)(lambda: c_own(k - 1))
        pl.when(k > 1)(lambda: chain(k - 2))
        return carry

    lax.fori_loop(0, deep, step, 0)
    chain(jnp.int32(deep - 2))
    last = jnp.int32(deep - 1)
    c_own(last)

    def add_line(make, side):
        make(last).wait_recv()
        own[OWN, last] += in_z[side, z].astype(jnp.float32)

    pl.when(z > 0)(lambda: add_line(line_up, 0))
    pl.when(z < deep - 1)(lambda: add_line(line_down, 1))
    out_ref[...] = own[OWN, last].astype(out_ref.dtype)

    def drain(k, carry):
        for kind in (DIAG, DY, DX, OWN):
            sib(kind, k).wait_send()
        for make in (half_x, half_y, whole_x, whole_y):
            make(k).wait_send()
        pl.when(dest(k) > z)(lambda: line_up(k).wait_send())
        pl.when(dest(k) < z)(lambda: line_down(k).wait_send())
        return carry

    lax.fori_loop(0, deep, drain, 0)


def kernels(layer_input, out_grad, route, gate_share, gate_weight, up_weight, down_weight):
    groups, members = lax.axis_size("ep"), lax.axis_size("tp")
    deep = members // 2
    rows, width = layer_input.shape
    hidden = gate_weight.shape[2]
    tiles = hidden // TILE
    chips = groups // CORES
    experts = jnp.arange(8, dtype=jnp.int32)
    shares = jnp.sum(
        jnp.where(route.T[None, :, :] == experts[:, None, None], gate_share.T[None, :, :], 0.0), axis=1)
    gate_matrix, up_matrix, down_matrix = gate_weight[0], up_weight[0], down_weight[0]
    anywhere = pl.BlockSpec(memory_space=pl.ANY)
    local = pl.BlockSpec(memory_space=pltpu.VMEM)
    bf16, f32 = jnp.bfloat16, jnp.float32
    both = CORES * rows
    dma = pltpu.SemaphoreType.DMA
    acts, shares = pl.pallas_call(
        functools.partial(gather_kernel, deep),
        out_shape=(
            jax.ShapeDtypeStruct((chips, both, 2 * hidden), bf16),
            jax.ShapeDtypeStruct((groups, 8, rows), f32),
        ),
        in_specs=[anywhere, anywhere, local, anywhere, anywhere, anywhere],
        out_specs=(anywhere, local),
        scratch_shapes=[
            pltpu.VMEM((members, chips, 2, both, width), bf16),
            pltpu.VMEM((3, 8, rows), f32),
            pltpu.VMEM((3, chips, tiles, both, TILE), f32),
            pltpu.VMEM((2, 2, width, hidden), bf16),
            pltpu.VMEM((2, hidden, width), bf16),
            pltpu.VMEM((chips, both, 2 * hidden), bf16),
            dma((5, members, chips, 2)),
            dma((2, members, chips, 2)),
            dma((members, 2)),
            dma((2, 3)),
            dma((2,)),
            dma((2, 3)),
            dma((chips,)),
        ],
        compiler_params=pltpu.CompilerParams(
            collective_id=0, has_side_effects=True, vmem_limit_bytes=VMEM_BYTES),
        name="gather",
    )(layer_input, out_grad, shares, gate_matrix, up_matrix, down_matrix)
    return pl.pallas_call(
        functools.partial(scatter_kernel, deep),
        out_shape=jax.ShapeDtypeStruct((rows, width), bf16),
        in_specs=[anywhere, local, anywhere, anywhere],
        out_specs=local,
        scratch_shapes=[
            pltpu.VMEM((chips, both, 2 * hidden), bf16),
            pltpu.VMEM((2, width, 2 * hidden), bf16),
            pltpu.VMEM((groups, rows, 128), f32),
            pltpu.VMEM((4, deep, rows, width), f32),
            pltpu.VMEM((4, deep, rows, width), bf16),
            pltpu.VMEM((4, deep, rows, width), bf16),
            pltpu.VMEM((4, deep, rows, width), bf16),
            pltpu.VMEM((deep, rows, width), bf16),
            pltpu.VMEM((deep, rows, width), bf16),
            pltpu.VMEM((deep, rows, width), bf16),
            pltpu.VMEM((2, deep, rows, width), bf16),
            dma((9, deep)),
            dma((8, deep)),
            dma((2, deep)),
            dma((chips, 2)),
            dma((2, 2)),
        ],
        compiler_params=pltpu.CompilerParams(
            collective_id=1, has_side_effects=True, vmem_limit_bytes=VMEM_BYTES),
        name="scatter",
    )(acts, shares, gate_matrix, up_matrix)


def permutes(layer_input, out_grad, route, gate_share, gate_weight, up_weight, down_weight):
    groups = lax.axis_size("ep")
    me = lax.axis_index("ep")
    chips = groups // CORES
    rows = layer_input.shape[0]
    gate_matrix = gate_weight[0]
    up_matrix = up_weight[0]
    down_matrix = down_weight[0]

    def shift(value, step):
        pairs = [(i, (i + step * CORES) % groups) for i in range(groups)]
        return lax.ppermute(value, "ep", pairs)

    def swap(value):
        return lax.ppermute(value, "ep", [(i, i ^ 1) for i in range(groups)])

    members = lax.axis_size("tp")
    inner = 1
    while 4 * inner * inner <= members:
        inner *= 2
    outer = members // inner
    place = lax.axis_index("tp")
    place_outer, place_inner = place // inner, place % inner
    width = layer_input.shape[1]

    def turn(value, outer_step, inner_step):
        pairs = []
        for i in range(members):
            target = (i // inner + outer_step) % outer * inner + (i % inner + inner_step) % inner
            pairs.append((i, target))
        return lax.ppermute(value, "tp", pairs)

    def gather(value):
        line = jnp.stack([value] + [turn(value, a, 0) for a in range(1, outer)])
        return jnp.concatenate([line] + [turn(line, 0, b) for b in range(1, inner)])

    def in_order(blocks):
        both = jnp.concatenate([blocks, swap(blocks)], axis=1)
        full = jnp.zeros((both.shape[1], members * width), both.dtype)
        for b in range(inner):
            for a in range(outer):
                source = (place_outer - a) % outer * inner + (place_inner - b) % inner
                full = lax.dynamic_update_slice(full, both[b * outer + a], (0, source * width))
        return full

    def scatter(value):
        def blocks_for(b):
            owner = (place_inner + b) % inner
            return [
                lax.dynamic_slice_in_dim(
                    value, ((place_outer + a) % outer * inner + owner) * width, width, axis=1
                )
                for a in range(outer)
            ]

        lines = jnp.stack(blocks_for(0))
        for b in range(1, inner):
            sent = jnp.stack(blocks_for(b)).astype(jnp.bfloat16)
            lines = lines + turn(sent, 0, b).astype(jnp.float32)
        result = lines[0]
        for a in range(1, outer):
            sent = turn(lines[a].astype(jnp.bfloat16), a, 0)
            result = result + sent.astype(jnp.float32)
        return result

    experts = jnp.arange(groups, dtype=jnp.int32)
    shares = jnp.sum(
        jnp.where(route[:, :, None] == experts, gate_share[:, :, None], 0.0), axis=1
    )

    gathered = []
    for step in range(chips):
        if step:
            part_input, part_grad = shift(layer_input, step), shift(out_grad, step)
            part_share = shift(shares, step)
        else:
            part_input, part_grad, part_share = layer_input, out_grad, shares
        full_input = gather(part_input)
        full_grad = gather(part_grad)
        share = jnp.concatenate([part_share, swap(part_share)], axis=0)
        share = jnp.sum(jnp.where(experts == me, share, 0.0), axis=1, keepdims=True)
        gathered.append((full_input, full_grad, share))

    total = None
    for step in range(chips):
        full_input, full_grad, share = gathered[step]
        inputs = in_order(full_input)
        grads = in_order(full_grad)
        gate_sum = jnp.dot(inputs, gate_matrix, preferred_element_type=jnp.float32)
        up_sum = jnp.dot(inputs, up_matrix, preferred_element_type=jnp.float32)
        hidden_sum = lax.dot_general(
            grads, down_matrix, (((1,), (1,)), ((), ())), preferred_element_type=jnp.float32
        )
        sigma = jax.nn.sigmoid(gate_sum)
        slope = sigma * (1.0 + gate_sum * (1.0 - sigma))
        gate_grad = (hidden_sum * up_sum * slope).astype(jnp.bfloat16)
        up_grad = (hidden_sum * gate_sum * sigma).astype(jnp.bfloat16)
        partial = lax.dot_general(
            gate_grad, gate_matrix, (((1,), (1,)), ((), ())), preferred_element_type=jnp.float32
        )
        partial = partial + lax.dot_general(
            up_grad, up_matrix, (((1,), (1,)), ((), ())), preferred_element_type=jnp.float32
        )
        partial = jnp.where(share > 0.0, partial * share, 0.0)
        other = swap(partial[rows:].astype(jnp.bfloat16))
        summed = scatter(partial[:rows] + other.astype(jnp.float32))
        if step:
            summed = shift(summed.astype(jnp.bfloat16), chips - step).astype(jnp.float32)
        total = summed if total is None else total + summed
    return total.astype(jnp.bfloat16)


def solution(mesh):
    groups, members = mesh.shape["ep"], mesh.shape["tp"]
    fits = groups == 2 * CORES and members == 8
    return jax.shard_map(
        kernels if fits else permutes,
        mesh=mesh,
        in_specs=(
            P("ep", "tp"),
            P("ep", "tp"),
            P("ep", None),
            P("ep", None),
            P("ep", None, "tp"),
            P("ep", None, "tp"),
            P("ep", "tp", None),
        ),
        out_specs=P("ep", "tp"),
        check_vma=False,
    )
```

```python
import functools

import jax
import jax.numpy as jnp
from jax import lax
from jax.experimental import pallas as pl
from jax.experimental.pallas import tpu as pltpu
from jax.sharding import PartitionSpec as P

CORES = 2
TILE = 256
VMEM_BYTES = 67_043_328
NT = (((1,), (1,)), ((), ()))
MESH = pl.DeviceIdType.MESH
UP, DOWN, ACROSS_X, ACROSS_Y, SIBLING, ACROSS_BOTH = range(6)

INNER_PLAN = (
    ("col", 0), ("dx", 0, 0), ("col", 2, 0), ("col", 1, 0), ("dy", 0, 0), ("col", 2, 1), ("col", 1, 1), ("cross", 1, 1), ("dx", 0, 1), ("dy", 0, 1),
    ("dy", 0), ("col", 3, 0), ("cross", 1, 0), ("dx", 1, 1), ("cross", 2, 1),
    ("col", 1), ("col", 3, 1), ("cross", 2, 0), ("diag", 0, 0), ("dy", 1, 1), ("diag", 0, 1),
    ("diag", 0),
    ("dx", 0), ("dy", 1, 0), ("dx", 1, 0),
    ("col", 2),
    ("col", 3), ("dy", 2, 1),
    ("dy", 1), ("diag", 2, 0), ("dx", 2, 1), ("cross", 3, 0), ("diag", 1, 0), ("dx", 2, 0),
    ("dx", 1), ("dy", 2, 0),
    ("dx", 2), ("diag", 1, 1), ("cross", 3, 1),
    ("dy", 2), ("diag", 2, 1),
    ("diag", 1), ("diag", 3, 0), ("dx", 3, 0),
    ("diag", 2), ("dx", 3, 1), ("dy", 3, 0), ("dy", 3, 1),
    ("dy", 3), ("diag", 3, 1),
    ("dx", 3),
    ("diag", 3),
)
OUTER_PLAN = (
    ("col", 0), ("dx", 0, 0), ("col", 1, 0), ("dy", 0, 0), ("dy", 0, 1), ("col", 1, 1), ("dx", 0, 1), ("cross", 1, 0),
    ("dy", 0), ("diag", 0, 1), ("cross", 1, 1), ("col", 2, 0),
    ("dx", 0), ("col", 2, 1), ("diag", 0, 0),
    ("col", 1), ("dx", 1, 0), ("cross", 2, 0), ("dy", 1, 0),
    ("col", 2), ("cross", 2, 1),
    ("diag", 0), ("col", 3, 0), ("dy", 1, 1), ("dx", 1, 1), ("col", 3, 1),
    ("dy", 1), ("cross", 3, 1),
    ("col", 3), ("dx", 2, 0), ("diag", 1, 0), ("cross", 3, 0), ("dy", 2, 0), ("dx", 2, 1),
    ("dx", 1), ("dy", 2, 1), ("diag", 1, 1),
    ("dx", 2),
    ("diag", 1), ("diag", 2, 0),
    ("dy", 2), ("dx", 3, 1), ("dy", 3, 1), ("dy", 3, 0), ("dx", 3, 0),
    ("dy", 3), ("diag", 2, 1),
    ("dx", 3), ("diag", 3, 0), ("diag", 3, 1),
    ("diag", 2),
    ("diag", 3),
)


def pick(table, index):
    value = jnp.int32(table[-1])
    for i in range(len(table) - 1):
        value = jnp.where(index == i, jnp.int32(table[i]), value)
    return value


class Place:
    def __init__(self, deep):
        ep, tp = lax.axis_index("ep"), lax.axis_index("tp")
        self.deep = deep
        self.x, self.core = ep // CORES, ep % CORES
        self.z, self.y = tp // 2, tp % 2
        self.ep, self.tp = ep, tp

    def device(self, way):
        ep, tp = self.ep, self.tp
        if way == SIBLING:
            return (self.x * CORES + 1 - self.core, tp)
        if way == ACROSS_X:
            return ((1 - self.x) * CORES + self.core, tp)
        if way == ACROSS_BOTH:
            return ((1 - self.x) * CORES + 1 - self.core, tp)
        if way == ACROSS_Y:
            return (ep, self.z * 2 + 1 - self.y)
        return (ep, tp + 2 if way == UP else tp - 2)

    def greet(self):
        barrier = pltpu.get_barrier_semaphore()

        def signal(way):
            pl.semaphore_signal(barrier, inc=1, device_id=self.device(way), device_id_type=MESH)

        ways = (SIBLING, ACROSS_X, ACROSS_Y, ACROSS_BOTH)
        for way in ways:
            signal(way)
        pl.when(self.z < self.deep - 1)(lambda: signal(UP))
        pl.when(self.z > 0)(lambda: signal(DOWN))
        lines = (self.z > 0).astype(jnp.int32) + (self.z < self.deep - 1).astype(jnp.int32)
        pl.semaphore_wait(barrier, len(ways) + lines)


def near_first(deep):
    return [sorted(range(deep), key=lambda other: (abs(other - z), other)) for z in range(deep)]


def gather_kernel(deep, x_ref, g_ref, s_ref, wg_ref, wu_ref, wd_ref, act_ref, share_ref,
                  land, share_land, acc, weights_a, weights_d, stage,
                  send, recv, half, share_sems, own_sems, weight_sems, out_sems):
    here = Place(deep)
    x, y, z, core = here.x, here.y, here.z, here.core
    rows, width = x_ref.shape
    hidden = wg_ref.shape[1]
    tiles = hidden // TILE
    middle = rows // 2
    near = near_first(deep)
    zs = [z] + [pick([near[i][k] for i in range(deep)], z) for k in range(1, deep)]

    def at(kind, k):
        dx, dy = {"col": (0, 0), "dx": (1, 0), "dy": (0, 1), "diag": (1, 1)}[kind]
        return zs[k] * 2 + (1 - y if dy else y), (1 - x if dx else x)

    def copy(spot, a, way, part=None):
        p, xx = spot
        if part is None:
            rng = pl.ds(core * rows, rows)
        else:
            rng = pl.ds(core * rows + part * middle, middle)
        ref = land.at[p, xx, a, rng, :]
        who = 1 if way == SIBLING else 0
        arrive = half.at[p, a] if part == 1 else recv.at[who, p, xx, a]
        return pltpu.make_async_remote_copy(
            src_ref=ref, dst_ref=ref, send_sem=send.at[way, p, xx, a], recv_sem=arrive,
            device_id=here.device(way), device_id_type=MESH)

    def wait_in(spot, a, part=None):
        copy(spot, a, ACROSS_X, part).wait_recv()

    def wait_sibling(spot, a):
        p, xx = spot
        ref = land.at[p, xx, a, pl.ds((1 - core) * rows, rows), :]
        pltpu.make_async_remote_copy(
            src_ref=ref, dst_ref=ref, send_sem=send.at[SIBLING, p, xx, a], recv_sem=recv.at[1, p, xx, a],
            device_id=here.device(SIBLING), device_id_type=MESH).wait_recv()

    inner = jnp.logical_and(z > 0, z < deep - 1)
    outer = jnp.logical_not(inner)
    sent = []

    def guarded(k, way, go):
        if way == UP:
            pl.when(jnp.logical_and(z < deep - 1, zs[k] <= z))(go)
        elif way == DOWN:
            pl.when(jnp.logical_and(z > 0, zs[k] >= z))(go)
        else:
            go()

    def start(kind, k, a, way, part=None):
        sent.append((kind, k, a, way, part))
        guarded(k, way, lambda: copy(at(kind, k), a, way, part).start())

    def finish_sends():
        for kind, k, a, way, part in dict.fromkeys(sent):
            guarded(k, way, lambda: copy(at(kind, k), a, way, part).wait_send())

    def col(k, a):
        if k > 0:
            wait_in(at("col", k), a)
        start("col", k, a, UP)
        start("col", k, a, DOWN)
        start("col", k, a, SIBLING)

    def cross(k, a):
        start("col", k, a, ACROSS_X)
        start("col", k, a, ACROSS_Y)

    def dx(k, a):
        wait_in(at("dx", k), a)
        if a == 1 or k == 0:
            start("dx", k, a, ACROSS_Y, part=1)
        start("dx", k, a, SIBLING)

    def dy(k, a):
        wait_in(at("dy", k), a)
        if a == 1 or k == 0:
            start("dy", k, a, ACROSS_X, part=0)
        start("dy", k, a, SIBLING)

    def diag(k, a):
        split = a == 1 or k == 0
        wait_in(at("diag", k), a, part=0 if split else None)
        if split:
            wait_in(at("diag", k), a, part=1)
        if a == 0:
            start("diag", k, a, UP)
            start("diag", k, a, DOWN)
        start("diag", k, a, SIBLING)

    tasks_of = {"col": col, "cross": cross, "dx": dx, "dy": dy, "diag": diag}
    sides = []
    for plan, cond in ((INNER_PLAN, inner), (OUTER_PLAN, outer)):
        order, events = [], {}
        for name, k, *a in plan:
            if a:
                events.setdefault(len(order) - 1, []).append((tasks_of[name], k, a[0]))
            else:
                order.append((name, k))
        last = [max(i for i, (kind, _) in enumerate(order) if (kind in ("dx", "diag")) == far) for far in (False, True)]
        sides.append((order, events, last, cond))
    count = len(sides[0][0])

    def choose(entry, i):
        values = [pick([int(entry(unit)) for unit in order], i) for order, _, _, _ in sides]
        return jnp.where(inner, values[0], values[1])

    def spot_of(i):
        plane = zs[-1]
        step = choose(lambda unit: unit[1], i)
        for k in range(deep - 1):
            plane = jnp.where(step == k, zs[k], plane)
        turned_x = choose(lambda unit: unit[0] in ("dx", "diag"), i)
        turned_y = choose(lambda unit: unit[0] in ("dy", "diag"), i)
        return plane * 2 + (y + turned_y) % 2, (x + turned_x) % 2

    def load(i):
        p, _ = spot_of(i)
        band = pl.ds(p * width, width)
        slot = i % 2
        return [
            pltpu.make_async_copy(wg_ref.at[band, :], weights_a.at[slot, 0], weight_sems.at[slot, 0]),
            pltpu.make_async_copy(wu_ref.at[band, :], weights_a.at[slot, 1], weight_sems.at[slot, 1]),
            pltpu.make_async_copy(wd_ref.at[:, band], weights_d.at[slot], weight_sems.at[slot, 2]),
        ]

    own = at("col", 0)
    mine = pl.ds(core * rows, rows)
    fetch = [
        pltpu.make_async_copy(x_ref, land.at[own[0], own[1], 0, mine, :], own_sems.at[0]),
        pltpu.make_async_copy(g_ref, land.at[own[0], own[1], 1, mine, :], own_sems.at[1]),
    ]
    for c in fetch:
        c.start()
    for i in (0, 1):
        for c in load(jnp.int32(i)):
            c.start()
    here.greet()
    for c in fetch:
        c.wait()

    shares = []
    for i, way in enumerate((SIBLING, ACROSS_X, ACROSS_BOTH)):
        shares.append(pltpu.make_async_remote_copy(
            src_ref=s_ref, dst_ref=share_land.at[i], send_sem=share_sems.at[0, i],
            recv_sem=share_sems.at[1, i], device_id=here.device(way), device_id_type=MESH))
        shares[-1].start()
    for a in (0, 1):
        col(0, a)
        cross(0, a)

    def clear(n, carry):
        for xx in range(acc.shape[1]):
            for j in range(3):
                acc[j, xx, n] = jnp.zeros(acc.shape[3:], acc.dtype)
        return carry

    lax.fori_loop(0, tiles, clear, 0)

    def store(xx, n):
        spans = [pl.ds(pl.multiple_of(j * hidden + n * TILE, TILE), TILE) for j in (0, 1)]
        return [
            pltpu.make_async_copy(stage.at[xx, :, span], act_ref.at[xx, :, span], out_sems.at[xx, n, j])
            for j, span in enumerate(spans)
        ]

    def finish(xx):
        def body(n, carry):
            cols = pl.ds(pl.multiple_of(n * TILE, TILE), TILE)
            later = pl.ds(pl.multiple_of(hidden + n * TILE, TILE), TILE)
            gate, up, back = acc[0, xx, n], acc[1, xx, n], acc[2, xx, n]
            sigma = 0.5 * jnp.tanh(0.5 * gate) + 0.5
            scaled = back * sigma
            stage[xx, :, cols] = (scaled * up * (1.0 + gate * (1.0 - sigma))).astype(jnp.bfloat16)
            stage[xx, :, later] = (scaled * gate).astype(jnp.bfloat16)
            for c in store(xx, n):
                c.start()
            return carry

        lax.fori_loop(0, tiles, body, 0)

    def unit(i, carry):
        p, xx = spot_of(i)
        slot = i % 2
        wait_sibling((p, xx), 0)
        wait_sibling((p, xx), 1)
        for c in load(i):
            c.wait()
        for n in range(tiles):
            cols = pl.ds(n * TILE, TILE)
            acc[0, xx, n] += jnp.dot(
                land[p, xx, 0], weights_a[slot, 0, :, cols], preferred_element_type=jnp.float32)
            acc[1, xx, n] += jnp.dot(
                land[p, xx, 0], weights_a[slot, 1, :, cols], preferred_element_type=jnp.float32)
            acc[2, xx, n] += lax.dot_general(
                land[p, xx, 1], weights_d[slot, cols, :], NT, preferred_element_type=jnp.float32)

        @pl.when(i + 2 < count)
        def _():
            for c in load(i + 2):
                c.start()

        for order, events, last, cond in sides:
            for when, tasks in events.items():
                @pl.when(jnp.logical_and(i == when, cond))
                def _(tasks=tasks):
                    for task, k, a in tasks:
                        task(k, a)

        ends = [jnp.where(inner, sides[0][2][far], sides[1][2][far]) for far in (0, 1)]
        pl.when(i == ends[0])(lambda: finish(x))
        pl.when(i == ends[1])(lambda: finish(1 - x))
        return carry

    lax.fori_loop(0, count, unit, 0)
    share_ref[here.ep] = s_ref[...]
    for i, way in enumerate((SIBLING, ACROSS_X, ACROSS_BOTH)):
        shares[i].wait()
        share_ref[here.device(way)[0]] = share_land[i]
    def stored(n, carry):
        for xx in (x, 1 - x):
            for c in store(xx, n):
                c.wait()
        return carry

    lax.fori_loop(0, tiles, stored, 0)
    finish_sends()


DIAG, DY, DX, OWN = range(4)
HALF_X, HALF_Y, WHOLE_Y, WHOLE_X, ALONG_Z = range(4, 9)


def scatter_kernel(deep, act_ref, share_ref, wg_ref, wu_ref, out_ref,
                   acts, weights, share_cols, own, sib_out, sib_in, blocks, in_half, in_x, in_y, in_z,
                   send, recv, recv_z, act_sems, weight_sems):
    here = Place(deep)
    x, y, z, core = here.x, here.y, here.z, here.core
    rows, width = out_ref.shape
    hidden = wg_ref.shape[1]
    middle = rows // 2
    far = [line[::-1] for line in near_first(deep)]
    dests = [pick([far[i][k] for i in range(deep)], z) for k in range(deep - 1)] + [z]

    def dest(k):
        value = dests[-1]
        for j in range(deep - 1):
            value = jnp.where(k == j, dests[j], value)
        return value

    def load(k, same):
        band = pl.ds((dest(k) * 2 + (y if same else 1 - y)) * width, width)
        return [
            pltpu.make_async_copy(
                ref.at[band, :], weights.at[same, :, pl.ds(j * hidden, hidden)], weight_sems.at[same, j])
            for j, ref in enumerate((wg_ref, wu_ref))
        ]

    def fetch(xx):
        return [
            pltpu.make_async_copy(
                act_ref.at[xx, pl.ds(block * rows, rows)], acts.at[xx, pl.ds(j * rows, rows)], act_sems.at[xx, j])
            for j, block in enumerate((1 - core, core))
        ]

    first, zero = fetch(1 - x) + load(jnp.int32(0), 0), jnp.int32(0)
    second = fetch(x) + load(zero, 1)
    for c in first:
        c.start()
    for b in range(share_ref.shape[0]):
        table = share_ref[b].T
        chosen = lax.broadcasted_iota(jnp.int32, table.shape, 1) == here.ep
        column = jnp.sum(jnp.where(chosen, table, 0.0), axis=1, keepdims=True)
        share_cols[b] = jnp.broadcast_to(column, share_cols.shape[1:])
    here.greet()
    for c in first:
        c.wait()
    for c in second:
        c.start()

    def remote(src, dst, kind, k, way, arrive=None):
        return pltpu.make_async_remote_copy(
            src_ref=src, dst_ref=dst, send_sem=send.at[kind, k],
            recv_sem=recv.at[kind, k] if arrive is None else arrive,
            device_id=here.device(way), device_id_type=MESH)

    low, high = pl.ds(0, middle), pl.ds(middle, middle)

    def sib(kind, k):
        return remote(sib_out.at[kind, k], sib_in.at[kind, k], kind, k, SIBLING)

    def half_x(k):
        return remote(blocks.at[DIAG, k, low], in_half.at[k, low], HALF_X, k, ACROSS_X)

    def half_y(k):
        return remote(blocks.at[DIAG, k, high], in_half.at[k, high], HALF_Y, k, ACROSS_Y)

    def whole_y(k):
        return remote(blocks.at[DY, k], in_y.at[k], WHOLE_Y, k, ACROSS_Y)

    def whole_x(k):
        return remote(blocks.at[DX, k], in_x.at[k], WHOLE_X, k, ACROSS_X)

    def line_up(k):
        return remote(blocks.at[OWN, k], in_z.at[0, dest(k)], ALONG_Z, k, UP, recv_z.at[0, dest(k)])

    def line_down(k):
        return remote(blocks.at[OWN, k], in_z.at[1, dest(k)], ALONG_Z, k, DOWN, recv_z.at[1, dest(k)])

    def begin(make, k, when=None):
        if when is None:
            make(k).start()
        else:
            pl.when(when)(lambda: make(k).start())

    def multiply(kind, k):
        xx = x if kind in (DY, OWN) else 1 - x
        value = lax.dot_general(
            acts[xx], weights[int(kind in (DX, OWN))], NT, preferred_element_type=jnp.float32)
        other = value[:rows] * share_cols[xx * CORES + 1 - core][:, :1]
        sib_out[kind, k] = other.astype(jnp.bfloat16)
        begin(lambda k: sib(kind, k), k)
        own[kind, k] = value[rows:] * share_cols[xx * CORES + core][:, :1]

    def c_diag(k):
        sib(DIAG, k).wait_recv()
        blocks[DIAG, k] = (own[DIAG, k] + sib_in[DIAG, k].astype(jnp.float32)).astype(jnp.bfloat16)
        begin(half_x, k)
        begin(half_y, k)

    def c_side(k, kind, arrived, part, whole):
        sib(kind, k).wait_recv()
        arrived(k).wait_recv()
        other = pl.ds(middle - part.start, middle)
        blocks[kind, k, other] = (
            own[kind, k, other] + sib_in[kind, k, other].astype(jnp.float32)).astype(jnp.bfloat16)
        blocks[kind, k, part] = (
            own[kind, k, part] + sib_in[kind, k, part].astype(jnp.float32)
            + in_half[k, part].astype(jnp.float32)).astype(jnp.bfloat16)
        begin(whole, k)

    def c_dy(k):
        c_side(k, DY, half_x, low, whole_y)

    def c_dx(k):
        c_side(k, DX, half_y, high, whole_x)

    def up_in(k):
        return jnp.logical_and(dest(k) > z, z > 0)

    def down_in(k):
        return jnp.logical_and(dest(k) < z, z < deep - 1)

    def pass_on(k, when):
        begin(line_up, k, jnp.logical_and(when, dest(k) > z))
        begin(line_down, k, jnp.logical_and(when, dest(k) < z))

    def c_own(k):
        sib(OWN, k).wait_recv()
        whole_x(k).wait_recv()
        whole_y(k).wait_recv()
        own[OWN, k] = (own[OWN, k] + sib_in[OWN, k].astype(jnp.float32)
                       + (in_x[k].astype(jnp.float32) + in_y[k].astype(jnp.float32)))

        @pl.when(k < deep - 1)
        def _():
            blocks[OWN, k] = own[OWN, k].astype(jnp.bfloat16)
            pass_on(k, jnp.logical_not(jnp.logical_or(up_in(k), down_in(k))))

    def chain(k):
        def add(make, side):
            make(k).wait_recv()
            blocks[OWN, k] = (own[OWN, k] + in_z[side, dest(k)].astype(jnp.float32)).astype(jnp.bfloat16)

        pl.when(up_in(k))(lambda: add(line_up, 0))
        pl.when(down_in(k))(lambda: add(line_down, 1))
        pass_on(k, jnp.logical_or(up_in(k), down_in(k)))

    def step(k, carry):
        @pl.when(k > 0)
        def _():
            for c in load(k, 0):
                c.wait()

        multiply(DIAG, k)

        @pl.when(k == 0)
        def _():
            for c in fetch(x):
                c.wait()

        @pl.when(k > 0)
        def _():
            multiply(OWN, k - 1)
            for c in load(k, 1):
                c.start()

        c_diag(k)
        multiply(DY, k)
        for c in load(k, 1):
            c.wait()

        @pl.when(k < deep - 1)
        def _():
            for c in load(k + 1, 0):
                c.start()

        multiply(DX, k)
        c_dy(k)
        c_dx(k)
        pl.when(k > 0)(lambda: c_own(k - 1))
        pl.when(k > 1)(lambda: chain(k - 2))
        return carry

    lax.fori_loop(0, deep, step, 0)
    multiply(OWN, jnp.int32(deep - 1))
    chain(jnp.int32(deep - 2))
    last = jnp.int32(deep - 1)
    c_own(last)

    def add_line(make, side):
        make(last).wait_recv()
        own[OWN, last] += in_z[side, z].astype(jnp.float32)

    pl.when(z > 0)(lambda: add_line(line_up, 0))
    pl.when(z < deep - 1)(lambda: add_line(line_down, 1))
    out_ref[...] = own[OWN, last].astype(out_ref.dtype)

    def drain(k, carry):
        for kind in (DIAG, DY, DX, OWN):
            sib(kind, k).wait_send()
        for make in (half_x, half_y, whole_x, whole_y):
            make(k).wait_send()
        pl.when(dest(k) > z)(lambda: line_up(k).wait_send())
        pl.when(dest(k) < z)(lambda: line_down(k).wait_send())
        return carry

    lax.fori_loop(0, deep, drain, 0)


def kernels(layer_input, out_grad, route, gate_share, gate_weight, up_weight, down_weight):
    groups, members = lax.axis_size("ep"), lax.axis_size("tp")
    deep = members // 2
    rows, width = layer_input.shape
    hidden = gate_weight.shape[2]
    tiles = hidden // TILE
    chips = groups // CORES
    experts = jnp.arange(8, dtype=jnp.int32)
    shares = jnp.sum(
        jnp.where(route.T[None, :, :] == experts[:, None, None], gate_share.T[None, :, :], 0.0), axis=1)
    gate_matrix, up_matrix, down_matrix = gate_weight[0], up_weight[0], down_weight[0]
    anywhere = pl.BlockSpec(memory_space=pl.ANY)
    local = pl.BlockSpec(memory_space=pltpu.VMEM)
    bf16, f32 = jnp.bfloat16, jnp.float32
    both = CORES * rows
    dma = pltpu.SemaphoreType.DMA
    acts, shares = pl.pallas_call(
        functools.partial(gather_kernel, deep),
        out_shape=(
            jax.ShapeDtypeStruct((chips, both, 2 * hidden), bf16),
            jax.ShapeDtypeStruct((groups, 8, rows), f32),
        ),
        in_specs=[anywhere, anywhere, local, anywhere, anywhere, anywhere],
        out_specs=(anywhere, local),
        scratch_shapes=[
            pltpu.VMEM((members, chips, 2, both, width), bf16),
            pltpu.VMEM((3, 8, rows), f32),
            pltpu.VMEM((3, chips, tiles, both, TILE), f32),
            pltpu.VMEM((2, 2, width, hidden), bf16),
            pltpu.VMEM((2, hidden, width), bf16),
            pltpu.VMEM((chips, both, 2 * hidden), bf16),
            dma((5, members, chips, 2)),
            dma((2, members, chips, 2)),
            dma((members, 2)),
            dma((2, 3)),
            dma((2,)),
            dma((2, 3)),
            dma((chips, tiles, 2)),
        ],
        compiler_params=pltpu.CompilerParams(
            collective_id=0, has_side_effects=True, vmem_limit_bytes=VMEM_BYTES),
        name="gather",
    )(layer_input, out_grad, shares, gate_matrix, up_matrix, down_matrix)
    return pl.pallas_call(
        functools.partial(scatter_kernel, deep),
        out_shape=jax.ShapeDtypeStruct((rows, width), bf16),
        in_specs=[anywhere, local, anywhere, anywhere],
        out_specs=local,
        scratch_shapes=[
            pltpu.VMEM((chips, both, 2 * hidden), bf16),
            pltpu.VMEM((2, width, 2 * hidden), bf16),
            pltpu.VMEM((groups, rows, 128), f32),
            pltpu.VMEM((4, deep, rows, width), f32),
            pltpu.VMEM((4, deep, rows, width), bf16),
            pltpu.VMEM((4, deep, rows, width), bf16),
            pltpu.VMEM((4, deep, rows, width), bf16),
            pltpu.VMEM((deep, rows, width), bf16),
            pltpu.VMEM((deep, rows, width), bf16),
            pltpu.VMEM((deep, rows, width), bf16),
            pltpu.VMEM((2, deep, rows, width), bf16),
            dma((9, deep)),
            dma((8, deep)),
            dma((2, deep)),
            dma((chips, 2)),
            dma((2, 2)),
        ],
        compiler_params=pltpu.CompilerParams(
            collective_id=1, has_side_effects=True, vmem_limit_bytes=VMEM_BYTES),
        name="scatter",
    )(acts, shares, gate_matrix, up_matrix)


def permutes(layer_input, out_grad, route, gate_share, gate_weight, up_weight, down_weight):
    groups = lax.axis_size("ep")
    me = lax.axis_index("ep")
    chips = groups // CORES
    rows = layer_input.shape[0]
    gate_matrix = gate_weight[0]
    up_matrix = up_weight[0]
    down_matrix = down_weight[0]

    def shift(value, step):
        pairs = [(i, (i + step * CORES) % groups) for i in range(groups)]
        return lax.ppermute(value, "ep", pairs)

    def swap(value):
        return lax.ppermute(value, "ep", [(i, i ^ 1) for i in range(groups)])

    members = lax.axis_size("tp")
    inner = 1
    while 4 * inner * inner <= members:
        inner *= 2
    outer = members // inner
    place = lax.axis_index("tp")
    place_outer, place_inner = place // inner, place % inner
    width = layer_input.shape[1]

    def turn(value, outer_step, inner_step):
        pairs = []
        for i in range(members):
            target = (i // inner + outer_step) % outer * inner + (i % inner + inner_step) % inner
            pairs.append((i, target))
        return lax.ppermute(value, "tp", pairs)

    def gather(value):
        line = jnp.stack([value] + [turn(value, a, 0) for a in range(1, outer)])
        return jnp.concatenate([line] + [turn(line, 0, b) for b in range(1, inner)])

    def in_order(blocks):
        both = jnp.concatenate([blocks, swap(blocks)], axis=1)
        full = jnp.zeros((both.shape[1], members * width), both.dtype)
        for b in range(inner):
            for a in range(outer):
                source = (place_outer - a) % outer * inner + (place_inner - b) % inner
                full = lax.dynamic_update_slice(full, both[b * outer + a], (0, source * width))
        return full

    def scatter(value):
        def blocks_for(b):
            owner = (place_inner + b) % inner
            return [
                lax.dynamic_slice_in_dim(
                    value, ((place_outer + a) % outer * inner + owner) * width, width, axis=1
                )
                for a in range(outer)
            ]

        lines = jnp.stack(blocks_for(0))
        for b in range(1, inner):
            sent = jnp.stack(blocks_for(b)).astype(jnp.bfloat16)
            lines = lines + turn(sent, 0, b).astype(jnp.float32)
        result = lines[0]
        for a in range(1, outer):
            sent = turn(lines[a].astype(jnp.bfloat16), a, 0)
            result = result + sent.astype(jnp.float32)
        return result

    experts = jnp.arange(groups, dtype=jnp.int32)
    shares = jnp.sum(
        jnp.where(route[:, :, None] == experts, gate_share[:, :, None], 0.0), axis=1
    )

    gathered = []
    for step in range(chips):
        if step:
            part_input, part_grad = shift(layer_input, step), shift(out_grad, step)
            part_share = shift(shares, step)
        else:
            part_input, part_grad, part_share = layer_input, out_grad, shares
        full_input = gather(part_input)
        full_grad = gather(part_grad)
        share = jnp.concatenate([part_share, swap(part_share)], axis=0)
        share = jnp.sum(jnp.where(experts == me, share, 0.0), axis=1, keepdims=True)
        gathered.append((full_input, full_grad, share))

    total = None
    for step in range(chips):
        full_input, full_grad, share = gathered[step]
        inputs = in_order(full_input)
        grads = in_order(full_grad)
        gate_sum = jnp.dot(inputs, gate_matrix, preferred_element_type=jnp.float32)
        up_sum = jnp.dot(inputs, up_matrix, preferred_element_type=jnp.float32)
        hidden_sum = lax.dot_general(
            grads, down_matrix, (((1,), (1,)), ((), ())), preferred_element_type=jnp.float32
        )
        sigma = jax.nn.sigmoid(gate_sum)
        slope = sigma * (1.0 + gate_sum * (1.0 - sigma))
        gate_grad = (hidden_sum * up_sum * slope).astype(jnp.bfloat16)
        up_grad = (hidden_sum * gate_sum * sigma).astype(jnp.bfloat16)
        partial = lax.dot_general(
            gate_grad, gate_matrix, (((1,), (1,)), ((), ())), preferred_element_type=jnp.float32
        )
        partial = partial + lax.dot_general(
            up_grad, up_matrix, (((1,), (1,)), ((), ())), preferred_element_type=jnp.float32
        )
        partial = jnp.where(share > 0.0, partial * share, 0.0)
        other = swap(partial[rows:].astype(jnp.bfloat16))
        summed = scatter(partial[:rows] + other.astype(jnp.float32))
        if step:
            summed = shift(summed.astype(jnp.bfloat16), chips - step).astype(jnp.float32)
        total = summed if total is None else total + summed
    return total.astype(jnp.bfloat16)


def solution(mesh):
    groups, members = mesh.shape["ep"], mesh.shape["tp"]
    fits = groups == 2 * CORES and members == 8
    return jax.shard_map(
        kernels if fits else permutes,
        mesh=mesh,
        in_specs=(
            P("ep", "tp"),
            P("ep", "tp"),
            P("ep", None),
            P("ep", None),
            P("ep", None, "tp"),
            P("ep", None, "tp"),
            P("ep", "tp", None),
        ),
        out_specs=P("ep", "tp"),
        check_vma=False,
    )
```
